256 devices in a mesh: gx: 16 (over y_hi, z), gy: 16 (over y_lo, x, core).
Axes of the slice: x: 4, y: 4 (y_hi: 2, y_lo: 2; y = y_hi * 2 + y_lo), z: 8, core: 2. Of those that a mesh axis runs over, the one named last changes fastest.
Arguments:
- hidden: bfloat16 [8192, 14336], P('gx', 'gy'), may hold values from -6 to 6
- weight: bfloat16 [4096, 14336], P(None, 'gy'), may hold values from -0.0625 to 0.0625
- cotangent: bfloat16 [8192, 4096], P('gx', 'gy'), may hold values from -6 to 6
Outputs:
- output: bfloat16 [8192, 4096], P('gx', 'gy')
- hidden_grad: bfloat16 [8192, 14336], P('gx', 'gy')
- weight_grad: float32 [4096, 14336], P('gx', 'gy')
The draws below stay inside these ranges and needn't reach their ends.
All inputs are finite; a program needn't handle non-finite values.
Results may differ from the reference program's by a relative error of at most 0.001.
Values may be sent and summed in bfloat16 or wider, within the bound.
No kernel may reach another device: no remote copies, remote signals or barrier semaphores. Data moves between devices by JAX's collectives and lax.ppermute only.
A program may use at most 128 MiB of HBM per device.

```python
import jax
import jax.numpy as jnp

D = 4096
FF = 14336
TOKENS = 8192


def strengthened(values, rng, source, target, blocks, factor):
    def block_of(position):
        return (jnp.arange(values.shape[position]) // (values.shape[position] // blocks)).reshape((-1,) + (1,) * (values.ndim - 1 - position))

    near = jax.random.permutation(rng, blocks)[block_of(target)]
    far = (block_of(target) + blocks // 2) % blocks
    return jnp.where((block_of(source) == near) | (block_of(source) == far), factor * values, values)


def block_scale(rng, dims, pieces, smallest, high):
    gain, own = 1.0, jax.random.fold_in(rng, 6)
    for position, blocks in pieces:
        heights = jnp.exp(jax.random.uniform(jax.random.fold_in(own, position), (blocks,), jnp.float32, smallest / len(pieces), high / len(pieces)))
        gain = gain * jnp.repeat(heights, dims[position] // blocks).reshape([-1 if axis == position else 1 for axis in range(len(dims))])
    return gain


def scatter_about(own_key, dims, spread, limit, shards=(), held_as=jnp.bfloat16):
    loudness = block_scale(own_key, dims, shards, -0.22, 0.18) if shards else 1.0
    values = jax.random.normal(own_key, dims, jnp.float32) * spread * loudness
    return jnp.minimum(jnp.maximum(values, -limit), limit).astype(held_as)


def gaussian_with(stream_key, shape, deviation, reach, split, heavy, kind=jnp.bfloat16):
    result = deviation * jax.random.normal(stream_key, shape, jnp.float32)
    if split:
        result = result * block_scale(stream_key, shape, split, -0.22, 0.18)
    return jnp.clip(strengthened(result, jax.random.fold_in(stream_key, 3), *heavy), -reach, reach).astype(kind)


def setup_inputs(seed: int = 0) -> dict:
    arg_keys = jax.random.split(jax.random.key(seed), 4)
    hidden = scatter_about(arg_keys[0], (TOKENS, FF), 1.0, 6.0, ((0, 16), (1, 16)))
    weight = gaussian_with(arg_keys[1], (D, FF), FF ** -0.5, 0.0625, ((1, 16),), (1, 0, 16, 2.0))
    cotangent = gaussian_with(arg_keys[2], (TOKENS, D), 1.0, 6.0, ((0, 16), (1, 16)), (0, 1, 16, 2.0))
    return {"hidden": hidden, "weight": weight, "cotangent": cotangent}


def reference(hidden, weight, cotangent):
    hidden_f = hidden.astype(jnp.float32)
    weight_f = weight.astype(jnp.float32)
    cotangent_f = cotangent.astype(jnp.float32)
    output = jnp.dot(hidden_f, weight_f.T, preferred_element_type=jnp.float32).astype(jnp.bfloat16)
    hidden_grad = jnp.dot(cotangent_f, weight_f, preferred_element_type=jnp.float32).astype(jnp.bfloat16)
    weight_grad = jnp.dot(cotangent_f.T, hidden_f, preferred_element_type=jnp.float32) * (TOKENS ** -0.5)
    return output, hidden_grad, weight_grad
```

```python
import jax
import jax.numpy as jnp
from jax import lax
from jax.experimental import pallas as pl
from jax.experimental.pallas import tpu as pltpu
from jax.sharding import Mesh
from jax.sharding import PartitionSpec as P


YH, Z, YL, X, C = "yh", "z", "yl", "x", "c"
F32, F16, BF16 = jnp.float32, jnp.float16, jnp.bfloat16
VMEM = pltpu.VMEM


def turned(axis, by):
    def move(array):
        n = lax.axis_size(axis)
        return lax.ppermute(array, axis, [(i, (i + by) % n) for i in range(n)])

    return move


z_up, z_down = turned(Z, 1), turned(Z, -1)
x_up, x_down = turned(X, 1), turned(X, -1)
other_core, other_yl, other_yh = turned(C, 1), turned(YL, 1), turned(YH, 1)


def pick(array, index):
    return lax.dynamic_index_in_dim(array, index, 0, keepdims=False)


def dot(a, b, da, db):
    return lax.dot_general(a, b, (((da,), (db,)), ((), ())), preferred_element_type=F32)


def cost(flops, bytes_accessed):
    return pl.CostEstimate(flops=flops, bytes_accessed=bytes_accessed, transcendentals=0)


def out_parts(hidden, hidden_c, weight, weight_c, order):
    t, u = hidden.shape
    n, r = order.shape[0], 256

    def kernel(order_ref, h_ref, hc_ref, w_ref, wc_ref, o_ref):
        o_ref[0] = dot(h_ref[...], w_ref[...], 1, 1) + dot(hc_ref[...], wc_ref[...], 1, 1)

    rows = pl.BlockSpec((r, u), lambda i, o: (o[i], 0))
    whole = pl.BlockSpec((t, u), lambda i, o: (0, 0))
    return pl.pallas_call(
        kernel,
        grid_spec=pltpu.PrefetchScalarGridSpec(
            num_scalar_prefetch=1,
            grid=(n,),
            in_specs=[whole, whole, rows, rows],
            out_specs=pl.BlockSpec((1, t, r), lambda i, o: (i, 0, 0)),
        ),
        out_shape=jax.ShapeDtypeStruct((n, t, r), F32),
        compiler_params=pltpu.CompilerParams(vmem_limit_bytes=58 << 20),
        cost_estimate=cost(4 * n * t * r * u, 4 * n * r * u + 4 * n * t * r),
        name="out_parts",
    )(order, hidden, hidden_c, weight, weight_c)


def grad_parts(mine, theirs, hidden, hidden2):
    n, _, t, r = mine.shape
    u = hidden.shape[1]

    def kernel(a_ref, b_ref, h_ref, h2_ref, o_ref):
        for p, ref in enumerate((a_ref, b_ref)):
            o_ref[0, p] = dot(ref[0, 0], h_ref[...], 0, 0) + dot(ref[0, 1], h2_ref[...], 0, 0)

    part = pl.BlockSpec((1, 2, t, r), lambda i: (i, 0, 0, 0))
    whole = pl.BlockSpec((t, u), lambda i: (0, 0))
    return pl.pallas_call(
        kernel,
        grid=(n,),
        in_specs=[part, part, whole, whole],
        out_specs=pl.BlockSpec((1, 2, r, u), lambda i: (i, 0, 0, 0)),
        out_shape=jax.ShapeDtypeStruct((n, 2, r, u), F32),
        compiler_params=pltpu.CompilerParams(vmem_limit_bytes=20 << 20),
        cost_estimate=cost(8 * n * t * r * u, 8 * n * t * r + 8 * n * r * u),
        name="grad_parts",
    )(mine, theirs, hidden, hidden2)


def hidden_gradient(blocks, weight, order):
    t, r = blocks[0].shape[1:]
    u = weight.shape[1]
    m = len(blocks)
    n = sum(b.shape[0] for b in blocks) // 4
    assert m == 4

    def kernel(order_ref, *refs):
        cots, ws, o_ref, acc_ref = refs[:m], refs[m : 2 * m], refs[2 * m], refs[2 * m + 1]
        i = pl.program_id(0)
        total = dot(cots[0][0], ws[0][...], 1, 0)
        for a in range(1, m):
            total += dot(cots[a][0], ws[a][...], 1, 0)

        @pl.when(i == 0)
        def _():
            acc_ref[...] = total

        @pl.when(i > 0)
        def _():
            acc_ref[...] += total

        @pl.when(i == n - 1)
        def _():
            o_ref[...] = acc_ref[...].astype(BF16)

    part = pl.BlockSpec((1, t, r), lambda i, o: (i, 0, 0))
    rows = [pl.BlockSpec((r, u), lambda i, o, a=a: (o[a * n + i], 0)) for a in range(m)]
    return pl.pallas_call(
        kernel,
        grid_spec=pltpu.PrefetchScalarGridSpec(
            num_scalar_prefetch=1,
            grid=(n,),
            in_specs=[part] * m + rows,
            out_specs=pl.BlockSpec((t, u), lambda i, o: (0, 0)),
            scratch_shapes=[VMEM((t, u), F32)],
        ),
        out_shape=jax.ShapeDtypeStruct((t, u), BF16),
        compiler_params=pltpu.CompilerParams(vmem_limit_bytes=20 << 20),
        cost_estimate=cost(2 * m * n * t * r * u, 2 * m * n * (t * r + r * u)),
        name="hidden_gradient",
    )(order, *blocks, *([weight] * m))


def layer(hidden, weight, cotangent):
    tokens, units = hidden.shape
    rows = cotangent.shape[1]
    scale = float(tokens * 16) ** -0.5
    yh, z, yl, x, c = (lax.axis_index(a) for a in (YH, Z, YL, X, C))

    sib = other_yl(cotangent)
    far = lax.ppermute(cotangent, (YH, YL), [(2, 0), (1, 3)])
    near = lax.ppermute(cotangent, (YH, YL), [(2, 1), (1, 2)])
    weight_c = other_core(weight)
    hidden_c = other_core(hidden)
    hidden2 = other_yh(hidden)
    own = yl == yh
    crit0 = jnp.where(own, cotangent, sib)
    crit1 = far + near
    rest = jnp.where(own, sib, cotangent)

    c0u = x_up(crit0)
    c1d = x_down(crit1)
    c1u = x_up(crit1)
    c0d = x_down(crit0)
    c0uu = x_up(c0u)
    c1dd = x_down(c1d)
    half_t = tokens // 2
    ru = x_up(rest)
    rd = x_down(rest)
    ruu = x_up(ru[:half_t])
    rdd = x_down(rd[half_t:])

    near_x = jnp.stack([jnp.stack(p) for p in ((crit0, crit1), (c0u, c1u), (c0d, c1d))])
    near_o = other_core(near_x)
    far_x = jnp.stack([c0uu, c1dd])[None]
    far_o = other_core(far_x)
    rest_x = jnp.stack([rest, ru, rd, jnp.concatenate([ruu, rdd], 0)])
    rest_o = other_core(rest_x)

    places = [(2, 0), (2, 1), (1, 0), (1, 1), (3, 0), (3, 1)]
    order = [y * 4 + (x + k) % 4 for k, y in places] + [yl * 4 + x, (1 - yl) * 4 + x]
    order = jnp.stack([k * 2 + c for k in order]).astype(jnp.int32)
    parts = out_parts(hidden, hidden_c, weight, weight_c, order)
    up = x_up(parts[0])
    down = x_down(parts[1])
    up = x_up(jnp.stack([parts[2] + up, parts[3]]))
    down = x_down(jnp.stack([parts[4], parts[5] + down]))
    give = parts[7] + (pick(up, 1 - yl) + pick(down, 1 - yl))
    keep = parts[6] + (pick(up, yl) + pick(down, yl))
    given = other_yl(give)
    output = (keep + given).astype(BF16)

    g_near = grad_parts(near_x, near_o, hidden, hidden2)
    g_far = grad_parts(far_x, far_o, hidden, hidden2)

    def grad_part(d):
        d = d % 8
        k = (x - d // 2) % 4
        p = (d + c) % 2
        at = jnp.where(k == 3, 2, jnp.where(k == 2, 0, k))
        near_d = lax.dynamic_slice(g_near, (at, p, 0, 0), (1, 1, rows, units))[0, 0]
        return jnp.where(k == 2, pick(g_far[0], p), near_d) * 0.25

    half = rows // 2
    g = grad_part(z + 4)
    up = z_up(g[:half].astype(F16))
    down = z_down(g[half:].astype(F16))
    for k in (3, 2, 1):
        gu = grad_part(z + k)
        gd = grad_part(z - k)
        if k == 3:
            gu = jnp.concatenate([gu[:half] + up.astype(F32), gu[half:]], 0)
            gd = jnp.concatenate([gd[:half], gd[half:] + down.astype(F32)], 0)
        else:
            gu, gd = gu + up.astype(F32), gd + down.astype(F32)
        up = z_up(gu.astype(F16))
        down = z_down(gd.astype(F16))
    weight_grad = (grad_part(z) + up.astype(F32) + down.astype(F32)) * (scale * 4.0)

    crit_x = jnp.concatenate([near_x[:, 0], far_x[:, 0]], 0)
    crit_o = jnp.concatenate([near_o[:, 0], far_o[:, 0]], 0)
    order = []
    for y, cc in ((yh, c), (yh, 1 - c), (1 - yh, c), (1 - yh, 1 - c)):
        for k in (0, 1, 3, 2):
            order.append(y * 8 + (x - k) % 4 * 2 + cc)
    order = jnp.stack(order).astype(jnp.int32)
    hidden_grad = hidden_gradient([crit_x, crit_o, rest_x, rest_o], weight, order)
    return output, hidden_grad, weight_grad


def solution(mesh):
    finer = Mesh(mesh.devices.reshape(2, 8, 2, 4, 2), (YH, Z, YL, X, C))
    gx, gy = (YH, Z), (YL, X, C)
    return jax.shard_map(
        layer,
        mesh=finer,
        in_specs=(P(gx, gy), P(None, gy), P(gx, gy)),
        out_specs=(P(gx, gy), P(gx, gy), P(gx, gy)),
        check_vma=False,
    )
```

```python
import jax
import jax.numpy as jnp
from jax import lax
from jax.experimental import pallas as pl
from jax.experimental.pallas import tpu as pltpu
from jax.sharding import Mesh
from jax.sharding import PartitionSpec as P


YH, Z, YL, X, C = "yh", "z", "yl", "x", "c"
F32, F16, BF16 = jnp.float32, jnp.float16, jnp.bfloat16
VMEM = pltpu.VMEM


def turned(axis, by):
    def move(array):
        n = lax.axis_size(axis)
        return lax.ppermute(array, axis, [(i, (i + by) % n) for i in range(n)])

    return move


def outward(axis):
    def move(array):
        n = lax.axis_size(axis)
        pairs = [((i, 0), ((i + 1) % n, 0)) for i in range(n)]
        pairs += [((i, 1), ((i - 1) % n, 1)) for i in range(n)]
        flat = [(a * 2 + p, b * 2 + q) for (a, p), (b, q) in pairs]
        return lax.ppermute(array, (axis, C), flat)

    return move


x_out, z_out = outward(X), outward(Z)
other_core, other_yl, other_yh = turned(C, 1), turned(YL, 1), turned(YH, 1)


def pick(array, index):
    return lax.dynamic_index_in_dim(array, index, 0, keepdims=False)


def dot(a, b, da, db):
    return lax.dot_general(a, b, (((da,), (db,)), ((), ())), preferred_element_type=F32)


def table(values):
    return jnp.array(values, jnp.int32)


def cost(flops, bytes_accessed):
    return pl.CostEstimate(flops=flops, bytes_accessed=bytes_accessed, transcendentals=0)


def out_parts(hidden, hidden_c, weight, weight_c, order):
    t, u = hidden.shape
    n, r = order.shape[0], 256

    def kernel(order_ref, h_ref, hc_ref, w_ref, wc_ref, *rest):
        outs, (h_t, rows, sums, sems, out_sems) = rest[:3], rest[3:]

        def fetch(i):
            at = pl.ds(pl.multiple_of(order_ref[i] * r, r), r)
            return [
                pltpu.make_async_copy(ref.at[at], rows.at[i, p], sems.at[i, p])
                for p, ref in enumerate((w_ref, wc_ref))
            ]

        for i in range(n):
            for copy in fetch(i):
                copy.start()
        h_t[0], h_t[1] = h_ref[...].T, hc_ref[...].T
        places = [out.at[i] for out in outs for i in range(out.shape[0])]
        for i in range(n):
            for copy in fetch(i):
                copy.wait()
            sums[i] = dot(rows[i, 0], h_t[0], 1, 0) + dot(rows[i, 1], h_t[1], 1, 0)
            pltpu.make_async_copy(sums.at[i], places[i], out_sems.at[i]).start()
        for i in range(n):
            pltpu.make_async_copy(sums.at[i], places[i], out_sems.at[i]).wait()

    vmem, hbm = pl.BlockSpec(memory_space=VMEM), pl.BlockSpec(memory_space=pltpu.HBM)
    return pl.pallas_call(
        kernel,
        in_specs=[pl.BlockSpec(memory_space=pltpu.SMEM), vmem, vmem, hbm, hbm],
        out_specs=[hbm] * 3,
        out_shape=[jax.ShapeDtypeStruct((k, r, t), F32) for k in (2, 4, 2)],
        scratch_shapes=[
            VMEM((2, u, t), BF16),
            VMEM((n, 2, r, u), BF16),
            VMEM((n, r, t), F32),
            pltpu.SemaphoreType.DMA((n, 2)),
            pltpu.SemaphoreType.DMA((n,)),
        ],
        compiler_params=pltpu.CompilerParams(vmem_limit_bytes=52 << 20),
        cost_estimate=cost(4 * n * t * r * u, 4 * n * t * r),
        name="out_parts",
    )(order, hidden, hidden_c, weight, weight_c)


def grad_parts(blocks, places, hiddens, first, count, own):
    _, t, r = blocks[0].shape
    u = hiddens[0].shape[1]
    m = len(blocks)
    half = first == 0
    rows = r // 2 if half else r

    def kernel(table_ref, *refs):
        blks, (h0, h1, k0, k1), outs = refs[:m], refs[m : m + 4], refs[m + 4 : -2]
        chosen, flipped = refs[-2:]

        def choose(j):
            for i, blk in enumerate(blks):

                @pl.when(table_ref[j] == i)
                def _():
                    if half:
                        for c in range(2):

                            @pl.when(table_ref[7] == c)
                            def _():
                                chosen[...] = blk[:, :, c * rows : (c + 1) * rows]
                    else:
                        chosen[...] = blk[...]

            for i in range(2):
                flipped[i] = chosen[i].T

        for j in range(count):
            choose(first + j)
            outs[0][j, 0] = dot(flipped[0], h0[...], 1, 0) + dot(flipped[1], h1[...], 1, 0)
            outs[0][j, 1] = dot(flipped[0], k0[...], 1, 0) + dot(flipped[1], k1[...], 1, 0)
        if own:
            choose(first + count)
            outs[1][...] = dot(flipped[0], h0[...], 1, 0) + dot(flipped[1], h1[...], 1, 0)

    shapes = [jax.ShapeDtypeStruct((count, 2, rows, u), F32)]
    if own:
        shapes.append(jax.ShapeDtypeStruct((r, u), F32))
    vmem = pl.BlockSpec(memory_space=VMEM)
    work = 4 * count + 2 * own
    return pl.pallas_call(
        kernel,
        in_specs=[pl.BlockSpec(memory_space=pltpu.SMEM)] + [vmem] * (m + 4),
        out_specs=[vmem] * len(shapes),
        out_shape=shapes,
        scratch_shapes=[VMEM((2, t, rows), BF16), VMEM((2, rows, t), BF16)],
        compiler_params=pltpu.CompilerParams(vmem_limit_bytes=18 << 20),
        cost_estimate=cost(2 * work * t * rows * u, 4 * work * rows * u),
        name="grad_parts",
    )(places, *blocks, *hiddens)


def hidden_gradient(blocks, weight, order):
    t, r = blocks[0].shape[1:]
    u = weight.shape[1]
    m = len(blocks)
    n = sum(b.shape[0] for b in blocks) // 4
    assert m == 4

    def kernel(order_ref, *refs):
        cots, ws, o_ref, acc_ref = refs[:m], refs[m : 2 * m], refs[2 * m], refs[2 * m + 1]
        i = pl.program_id(0)
        total = dot(cots[0][0], ws[0][...], 1, 0)
        for a in range(1, m):
            total += dot(cots[a][0], ws[a][...], 1, 0)

        @pl.when(i == 0)
        def _():
            acc_ref[...] = total

        @pl.when(i > 0)
        def _():
            acc_ref[...] += total

        @pl.when(i == n - 1)
        def _():
            o_ref[...] = acc_ref[...].astype(BF16)

    part = pl.BlockSpec((1, t, r), lambda i, o: (i, 0, 0))
    rows = [pl.BlockSpec((r, u), lambda i, o, a=a: (o[a * n + i], 0)) for a in range(m)]
    return pl.pallas_call(
        kernel,
        grid_spec=pltpu.PrefetchScalarGridSpec(
            num_scalar_prefetch=1,
            grid=(n,),
            in_specs=[part] * m + rows,
            out_specs=pl.BlockSpec((t, u), lambda i, o: (0, 0)),
            scratch_shapes=[VMEM((t, u), F32)],
        ),
        out_shape=jax.ShapeDtypeStruct((t, u), BF16),
        compiler_params=pltpu.CompilerParams(vmem_limit_bytes=14 << 20),
        cost_estimate=cost(2 * m * n * t * r * u, 2 * m * n * (t * r + r * u)),
        name="hidden_gradient",
    )(order, *blocks, *([weight] * m))


def layer(hidden, weight, cotangent):
    tokens, _ = hidden.shape
    rows = cotangent.shape[1]
    scale = float(tokens * 16) ** -0.5
    yh, z, yl, x, c = (lax.axis_index(a) for a in (YH, Z, YL, X, C))

    far = lax.ppermute(cotangent, (YH, YL), [(2, 0), (1, 3)])
    near = lax.ppermute(cotangent, (YH, YL), [(2, 1), (1, 2)])
    sib = other_yl(cotangent)
    hidden2 = other_yh(hidden)
    hidden_c = other_core(hidden)
    weight_c = other_core(weight)
    hidden2_c = other_core(hidden2)
    own = yl == yh
    crit = jnp.stack([jnp.where(own, cotangent, sib), far + near])
    rest = jnp.where(own, sib, cotangent)

    a1 = x_out(crit)
    crit_c = other_core(crit)
    a2 = x_out(crit_c)
    a3 = x_out(a1)
    b1 = other_core(a1)
    b2 = other_core(a2)
    b3 = other_core(a3)
    rest_c = other_core(rest)
    r1 = x_out(jnp.stack([rest, rest_c]))
    r2 = x_out(r1[0])
    r1_c = other_core(r1)
    r2_c = other_core(r2)

    ahead = 1 - 2 * c
    at_x = x + table([2, 2, 0, 0, 0, 0, 0, 0]) + ahead * table([0, 0, 1, 1, 1, 1, 0, 0])
    at_y = c * table([1, 1, 1, 1, 0, 0, 0, 0]) + (1 - c) * table([0, 0, 0, 0, 1, 1, 0, 0])
    at_y += yl * table([0, 0, 0, 0, 0, 0, 1, 0]) + (1 - yl) * table([0, 0, 0, 0, 0, 0, 0, 1])
    at_c = table([0, 1, 0, 1, 0, 1, 0, 0]) + c * table([0, 0, 0, 0, 0, 0, 1, 1])
    order = at_y * 8 + at_x % 4 * 2 + at_c
    first, following, last = out_parts(hidden, hidden_c, weight, weight_c, order)
    came = x_out(first)
    came = x_out(jnp.concatenate([following[:2] + came, following[2:]], 0))
    came = came.reshape(2, 2, rows, tokens)
    for_other = lax.dynamic_index_in_dim(came, 1 - c, 1, keepdims=False)
    from_other = other_core(for_other)
    for_own = lax.dynamic_index_in_dim(came, c, 1, keepdims=False)
    keep = last[0] + (pick(for_own, (yl + c) % 2) + pick(from_other, (yl + 1 + c) % 2))
    give = last[1] + (pick(for_own, (yl + 1 + c) % 2) + pick(from_other, (yl + c) % 2))
    given = other_yl(give)
    output = (keep + given).T.astype(BF16)

    blocks = [crit, crit_c, a1, a2, b2, b1, a3, b3]

    d = (z + ahead * table([4, 3, 2, 1, 0, 0, 0, 0])) % 8
    k = (x - d // 2) % 4
    at = jnp.where(k == 0, 0, jnp.where(k == 2, 6, jnp.where((k == 1) == (c == 0), 2, 4)))
    places = (at + (d + c) % 2) * table([1, 1, 1, 1, 1, 0, 0, 0]) + c * table([0, 0, 0, 0, 0, 1, 1, 1])
    hiddens = [hidden, hidden2, hidden_c, hidden2_c]
    (g0,) = grad_parts(blocks, places, hiddens, 0, 1, False)
    g, g_own = grad_parts(blocks, places, hiddens, 1, 3, True)
    came = z_out((g0[0] * 0.25).astype(F16))
    came = came.astype(F32)
    low = jnp.concatenate([jnp.where(c == 0, came, 0.0), jnp.where(c == 0, 0.0, came)], 1)
    came = z_out((g[0] * 0.25 + low).astype(F16))
    came = z_out((g[1] * 0.25 + came.astype(F32)).astype(F16))
    came = z_out((g[2] * 0.25 + came.astype(F32)).astype(F16))
    came_c = other_core(came)[1]
    weight_grad = g_own * scale + (came[0].astype(F32) + came_c.astype(F32)) * (scale * 4.0)

    mine = jnp.stack([crit[0], a1[0], b2[0], a3[0]])
    theirs = jnp.stack([crit_c[0], a2[0], b1[0], b3[0]])
    rest_m = jnp.stack([rest, r1[0], r1_c[1], r2])
    rest_t = jnp.stack([rest_c, r1[1], r1_c[0], r2_c])
    y = yh * table([1] * 8 + [0] * 8) + (1 - yh) * table([0] * 8 + [1] * 8)
    cc = c * table([1, 1, 1, 1, 0, 0, 0, 0] * 2) + (1 - c) * table([0, 0, 0, 0, 1, 1, 1, 1] * 2)
    order = y * 8 + (x + table([0, 0, 0, 2] * 4) + ahead * table([0, -1, 1, 0] * 4)) % 4 * 2 + cc
    hidden_grad = hidden_gradient([mine, theirs, rest_m, rest_t], weight, order)
    return output, hidden_grad, weight_grad


def solution(mesh):
    finer = Mesh(mesh.devices.reshape(2, 8, 2, 4, 2), (YH, Z, YL, X, C))
    gx, gy = (YH, Z), (YL, X, C)
    return jax.shard_map(
        layer,
        mesh=finer,
        in_specs=(P(gx, gy), P(None, gy), P(gx, gy)),
        out_specs=(P(gx, gy), P(gx, gy), P(gx, gy)),
        check_vma=False,
    )
```

```python
import jax
import jax.numpy as jnp
from jax import lax
from jax.experimental import pallas as pl
from jax.experimental.pallas import tpu as pltpu
from jax.sharding import Mesh
from jax.sharding import PartitionSpec as P


YH, Z, YL, X, C = "yh", "z", "yl", "x", "c"
F32, F16, BF16 = jnp.float32, jnp.float16, jnp.bfloat16
VMEM = pltpu.VMEM


def turned(axis, by):
    def move(array):
        n = lax.axis_size(axis)
        return lax.ppermute(array, axis, [(i, (i + by) % n) for i in range(n)])

    return move


def outward(axis):
    def move(array):
        n = lax.axis_size(axis)
        pairs = [((i, 0), ((i + 1) % n, 0)) for i in range(n)]
        pairs += [((i, 1), ((i - 1) % n, 1)) for i in range(n)]
        flat = [(a * 2 + p, b * 2 + q) for (a, p), (b, q) in pairs]
        return lax.ppermute(array, (axis, C), flat)

    return move


x_out, z_out = outward(X), outward(Z)
other_core, other_yl, other_yh = turned(C, 1), turned(YL, 1), turned(YH, 1)


def pick(array, index):
    return lax.dynamic_index_in_dim(array, index, 0, keepdims=False)


def dot(a, b, da, db):
    return lax.dot_general(a, b, (((da,), (db,)), ((), ())), preferred_element_type=F32)


def table(values):
    return jnp.array(values, jnp.int32)


def cost(flops, bytes_accessed):
    return pl.CostEstimate(flops=flops, bytes_accessed=bytes_accessed, transcendentals=0)


def out_parts(hidden, hidden_c, weight, weight_c, order):
    t, u = hidden.shape
    n, r = order.shape[0], 256

    def kernel(order_ref, h_ref, hc_ref, w_ref, wc_ref, *rest):
        outs, (h_t, rows, sums, sems, out_sems) = rest[:4], rest[4:]

        def fetch(i):
            at = pl.ds(pl.multiple_of(order_ref[i] * r, r), r)
            return [
                pltpu.make_async_copy(ref.at[at], rows.at[i, p], sems.at[i, p])
                for p, ref in enumerate((w_ref, wc_ref))
            ]

        for i in range(n):
            for copy in fetch(i):
                copy.start()
        h_t[0], h_t[1] = h_ref[...].T, hc_ref[...].T
        places = [out.at[i] for out in outs for i in range(out.shape[0])]
        for i in range(n):
            for copy in fetch(i):
                copy.wait()
            sums[i] = dot(rows[i, 0], h_t[0], 1, 0) + dot(rows[i, 1], h_t[1], 1, 0)
            pltpu.make_async_copy(sums.at[i], places[i], out_sems.at[i]).start()
        for i in range(n):
            pltpu.make_async_copy(sums.at[i], places[i], out_sems.at[i]).wait()

    vmem, hbm = pl.BlockSpec(memory_space=VMEM), pl.BlockSpec(memory_space=pltpu.HBM)
    return pl.pallas_call(
        kernel,
        in_specs=[pl.BlockSpec(memory_space=pltpu.SMEM), vmem, vmem, hbm, hbm],
        out_specs=[hbm] * 4,
        out_shape=[jax.ShapeDtypeStruct((k, r, t), F32) for k in (2, 2, 2, 2)],
        scratch_shapes=[
            VMEM((2, u, t), BF16),
            VMEM((n, 2, r, u), BF16),
            VMEM((n, r, t), F32),
            pltpu.SemaphoreType.DMA((n, 2)),
            pltpu.SemaphoreType.DMA((n,)),
        ],
        compiler_params=pltpu.CompilerParams(vmem_limit_bytes=52 << 20),
        cost_estimate=cost(4 * n * t * r * u, 4 * n * t * r),
        name="out_parts",
    )(order, hidden, hidden_c, weight, weight_c)


def grad_parts(blocks, places, hiddens, first, count, own):
    _, t, r = blocks[0].shape
    u = hiddens[0].shape[1]
    m = len(blocks)
    half = first == 0
    rows = r // 2 if half else r

    def kernel(table_ref, *refs):
        blks, (h0, h1, k0, k1), outs = refs[:m], refs[m : m + 4], refs[m + 4 : -2]
        chosen, flipped = refs[-2:]

        def choose(j):
            for i, blk in enumerate(blks):

                @pl.when(table_ref[j] == i)
                def _():
                    if half:
                        for c in range(2):

                            @pl.when(table_ref[7] == c)
                            def _():
                                chosen[...] = blk[:, :, c * rows : (c + 1) * rows]
                    else:
                        chosen[...] = blk[...]

            for i in range(2):
                flipped[i] = chosen[i].T

        for j in range(count):
            choose(first + j)
            outs[0][j, 0] = dot(flipped[0], h0[...], 1, 0) + dot(flipped[1], h1[...], 1, 0)
            outs[0][j, 1] = dot(flipped[0], k0[...], 1, 0) + dot(flipped[1], k1[...], 1, 0)
        if own:
            choose(first + count)
            outs[1][...] = dot(flipped[0], h0[...], 1, 0) + dot(flipped[1], h1[...], 1, 0)

    shapes = [jax.ShapeDtypeStruct((count, 2, rows, u), F32)]
    if own:
        shapes.append(jax.ShapeDtypeStruct((r, u), F32))
    vmem = pl.BlockSpec(memory_space=VMEM)
    work = 4 * count + 2 * own
    return pl.pallas_call(
        kernel,
        in_specs=[pl.BlockSpec(memory_space=pltpu.SMEM)] + [vmem] * (m + 4),
        out_specs=[vmem] * len(shapes),
        out_shape=shapes,
        scratch_shapes=[VMEM((2, t, rows), BF16), VMEM((2, rows, t), BF16)],
        compiler_params=pltpu.CompilerParams(vmem_limit_bytes=18 << 20),
        cost_estimate=cost(2 * work * t * rows * u, 4 * work * rows * u),
        name="grad_parts",
    )(places, *blocks, *hiddens)


def hidden_gradient(blocks, weight, order):
    t, r = blocks[0].shape[1:]
    u = weight.shape[1]
    m = len(blocks)
    n = sum(b.shape[0] for b in blocks) // 4
    assert m == 4

    def kernel(order_ref, *refs):
        cots, ws, o_ref, acc_ref = refs[:m], refs[m : 2 * m], refs[2 * m], refs[2 * m + 1]
        i = pl.program_id(0)
        total = dot(cots[0][0], ws[0][...], 1, 0)
        for a in range(1, m):
            total += dot(cots[a][0], ws[a][...], 1, 0)

        @pl.when(i == 0)
        def _():
            acc_ref[...] = total

        @pl.when(i > 0)
        def _():
            acc_ref[...] += total

        @pl.when(i == n - 1)
        def _():
            o_ref[...] = acc_ref[...].astype(BF16)

    part = pl.BlockSpec((1, t, r), lambda i, o: (i, 0, 0))
    rows = [pl.BlockSpec((r, u), lambda i, o, a=a: (o[a * n + i], 0)) for a in range(m)]
    return pl.pallas_call(
        kernel,
        grid_spec=pltpu.PrefetchScalarGridSpec(
            num_scalar_prefetch=1,
            grid=(n,),
            in_specs=[part] * m + rows,
            out_specs=pl.BlockSpec((t, u), lambda i, o: (0, 0)),
            scratch_shapes=[VMEM((t, u), F32)],
        ),
        out_shape=jax.ShapeDtypeStruct((t, u), BF16),
        compiler_params=pltpu.CompilerParams(vmem_limit_bytes=57 << 20),
        cost_estimate=cost(2 * m * n * t * r * u, 2 * m * n * (t * r + r * u)),
        name="hidden_gradient",
    )(order, *blocks, *([weight] * m))


def layer(hidden, weight, cotangent):
    tokens, _ = hidden.shape
    scale = float(tokens * 16) ** -0.5
    yh, z, yl, x, c = (lax.axis_index(a) for a in (YH, Z, YL, X, C))

    far = lax.ppermute(cotangent, (YH, YL), [(2, 0), (1, 3)])
    near = lax.ppermute(cotangent, (YH, YL), [(2, 1), (1, 2)])
    sib = other_yl(cotangent)
    hidden2 = other_yh(hidden)
    hidden_c = other_core(hidden)
    weight_c = other_core(weight)
    hidden2_c = other_core(hidden2)
    own = yl == yh
    crit = jnp.stack([jnp.where(own, cotangent, sib), far + near])
    rest = jnp.where(own, sib, cotangent)

    a1 = x_out(crit)
    crit_c = other_core(crit)
    a2 = x_out(crit_c)
    a3 = x_out(a1)
    b1 = other_core(a1)
    b2 = other_core(a2)
    b3 = other_core(a3)
    rest_c = other_core(rest)
    r1 = x_out(jnp.stack([rest, rest_c]))
    r2 = x_out(r1[0])
    r1_c = other_core(r1)
    r2_c = other_core(r2)

    ahead = 1 - 2 * c
    at_x = x + table([2, 2, 0, 0, 0, 0, 0, 0]) + ahead * table([0, 0, 1, 1, 1, 1, 0, 0])
    at_y = c * table([1, 1, 0, 0, 0, 0, 0, 0]) + yl * table([0, 0, 0, 0, 1, 1, 0, 1])
    at_y += (1 - yl) * table([0, 0, 1, 1, 0, 0, 1, 0])
    at_c = table([0, 1, 0, 1, 0, 1, 0, 0]) + c * table([0, 0, 0, 0, 0, 0, 1, 1])
    order = at_y * 8 + at_x % 4 * 2 + at_c
    first, give2, keep2, last = out_parts(hidden, hidden_c, weight, weight_c, order)
    came = x_out(first)
    gives = (yl != c).astype(F32)
    far_give = x_out(give2 + came * gives)
    far_keep = x_out(keep2 + came * (1.0 - gives))

    def both_cores(array):
        other = other_core(pick(array, 1 - c))
        return pick(array, c) + other

    give = both_cores(far_give)
    give = last[0] + give
    given = other_yl(give)
    keep = both_cores(far_keep)
    keep = last[1] + keep
    output = (keep + given).T.astype(BF16)

    blocks = [crit, crit_c, a1, a2, b2, b1, a3, b3]

    d = (z + ahead * table([4, 3, 2, 1, 0, 0, 0, 0])) % 8
    k = (x - d // 2) % 4
    at = jnp.where(k == 0, 0, jnp.where(k == 2, 6, jnp.where((k == 1) == (c == 0), 2, 4)))
    places = (at + (d + c) % 2) * table([1, 1, 1, 1, 1, 0, 0, 0]) + c * table([0, 0, 0, 0, 0, 1, 1, 1])
    hiddens = [hidden, hidden2, hidden_c, hidden2_c]
    (g0,) = grad_parts(blocks, places, hiddens, 0, 1, False)
    g, g_own = grad_parts(blocks, places, hiddens, 1, 3, True)
    came = z_out((g0[0] * 0.25).astype(F16))
    came = came.astype(F32)
    low = jnp.concatenate([jnp.where(c == 0, came, 0.0), jnp.where(c == 0, 0.0, came)], 1)
    came = z_out((g[0] * 0.25 + low).astype(F16))
    came = z_out((g[1] * 0.25 + came.astype(F32)).astype(F16))
    came = z_out((g[2] * 0.25 + came.astype(F32)).astype(F16))
    came_c = other_core(came)[1]
    weight_grad = g_own * scale + (came[0].astype(F32) + came_c.astype(F32)) * (scale * 4.0)

    mine = jnp.stack([crit[0], a1[0], b2[0], a3[0]])
    theirs = jnp.stack([crit_c[0], a2[0], b1[0], b3[0]])
    rest_m = jnp.stack([rest, r1[0], r1_c[1], r2])
    rest_t = jnp.stack([rest_c, r1[1], r1_c[0], r2_c])
    y = yh * table([1] * 8 + [0] * 8) + (1 - yh) * table([0] * 8 + [1] * 8)
    cc = c * table([1, 1, 1, 1, 0, 0, 0, 0] * 2) + (1 - c) * table([0, 0, 0, 0, 1, 1, 1, 1] * 2)
    order = y * 8 + (x + table([0, 0, 0, 2] * 4) + ahead * table([0, -1, 1, 0] * 4)) % 4 * 2 + cc
    hidden_grad = hidden_gradient([mine, theirs, rest_m, rest_t], weight, order)
    return output, hidden_grad, weight_grad


def solution(mesh):
    finer = Mesh(mesh.devices.reshape(2, 8, 2, 4, 2), (YH, Z, YL, X, C))
    gx, gy = (YH, Z), (YL, X, C)
    return jax.shard_map(
        layer,
        mesh=finer,
        in_specs=(P(gx, gy), P(None, gy), P(gx, gy)),
        out_specs=(P(gx, gy), P(gx, gy), P(gx, gy)),
        check_vma=False,
    )
```
